32 devices in a mesh: site: 2 (over core), replica: 4 (over z), model: 4 (over y, x).
Axes of the slice: x: 2, y: 2, z: 4, core: 2. Of those that a mesh axis runs over, the one named last changes fastest.
Arguments:
- partial_query: bfloat16 [8, 1024, 1024], P(('site', 'replica'), None, 'model'), parts along dimension 0, may hold values from -4 to 4
- partial_key: bfloat16 [8, 1024, 1024], P(('site', 'replica'), None, 'model'), parts along dimension 0, may hold values from -4 to 4
- partial_value: bfloat16 [8, 1024, 1024], P(('site', 'replica'), None, 'model'), parts along dimension 0, may hold values from -4 to 4
- partial_mixed: bfloat16 [8, 1024, 1024], P(('site', 'replica'), 'model'), parts along dimension 0, may hold values from -4 to 4
- partial_norm: bfloat16 [8, 1024], P(('site', 'replica')), parts along dimension 0, may hold values from -8 to 8
- master_query: float32 [2048, 1024], P(('site', 'replica'), 'model'), parts along dimension 0, may hold values from -0.1875 to 0.1875
- master_key: float32 [2048, 1024], P(('site', 'replica'), 'model'), parts along dimension 0, may hold values from -0.1875 to 0.1875
- master_value: float32 [2048, 1024], P(('site', 'replica'), 'model'), parts along dimension 0, may hold values from -0.1875 to 0.1875
- master_mixed: float32 [2048, 1024], P(('site', 'model'), 'replica'), parts along dimension 0, may hold values from -0.1875 to 0.1875
- master_norm: float32 [2048], P(('site', 'replica')), parts along dimension 0, may hold values from 0.25 to 1.75
- memory_query: float32 [2048, 1024], P(('site', 'replica'), 'model'), parts along dimension 0, may hold values from 0.05 to 0.8
- memory_key: float32 [2048, 1024], P(('site', 'replica'), 'model'), parts along dimension 0, may hold values from 0.05 to 0.8
- memory_value: float32 [2048, 1024], P(('site', 'replica'), 'model'), parts along dimension 0, may hold values from 0.05 to 0.8
- memory_mixed: float32 [2048, 1024], P(('site', 'model'), 'replica'), parts along dimension 0, may hold values from 0.05 to 0.8
- memory_norm: float32 [2048], P(('site', 'replica')), parts along dimension 0, may hold values from 0.05 to 0.8
Outputs:
- compute_query: bfloat16 [2048, 1024], P('site', 'model'), parts along dimension 0
- compute_key: bfloat16 [2048, 1024], P('site', 'model'), parts along dimension 0
- compute_value: bfloat16 [2048, 1024], P('site', 'model'), parts along dimension 0
- compute_mixed: bfloat16 [2048, 1024], P(('site', 'model')), parts along dimension 0
- compute_norm: bfloat16 [2048], P('site'), parts along dimension 0
- stepped_query: float32 [2048, 1024], P(('site', 'replica'), 'model'), parts along dimension 0
- stepped_key: float32 [2048, 1024], P(('site', 'replica'), 'model'), parts along dimension 0
- stepped_value: float32 [2048, 1024], P(('site', 'replica'), 'model'), parts along dimension 0
- stepped_mixed: float32 [2048, 1024], P(('site', 'model'), 'replica'), parts along dimension 0
- stepped_norm: float32 [2048], P(('site', 'replica')), parts along dimension 0
- state_new_query: float32 [2048, 1024], P(('site', 'replica'), 'model'), parts along dimension 0
- state_new_key: float32 [2048, 1024], P(('site', 'replica'), 'model'), parts along dimension 0
- state_new_value: float32 [2048, 1024], P(('site', 'replica'), 'model'), parts along dimension 0
- state_new_mixed: float32 [2048, 1024], P(('site', 'model'), 'replica'), parts along dimension 0
- state_new_norm: float32 [2048], P(('site', 'replica')), parts along dimension 0
The draws below stay inside these ranges and needn't reach their ends.
There are 2 independent parts, one for each index of `site`. The reference program is written for one: setup_inputs(seed, part) draws one part's arguments, and reference() takes and returns one part's arrays. A program takes and returns all parts, laid end to end along the dimension named above; each array names one. Nothing has to cross between parts.
All inputs are finite; a program needn't handle non-finite values.
Results may differ from the reference program's by a relative error of at most 0.001.
Values may be sent and summed in bfloat16 or wider, within the bound.
A program may use at most 64 MiB of HBM per device.

```python
import jax
import jax.numpy as jnp
from jax import lax

WIDTH = 1024
ATTN = 1024
REPLICAS = 4


def spiked(values, rng, source, target, blocks, factor):
    def block_of(axis_at):
        return (jnp.arange(values.shape[axis_at]) // (values.shape[axis_at] // blocks)).reshape((-1,) + (1,) * (values.ndim - 1 - axis_at))

    one_side = jax.random.permutation(rng, blocks)[block_of(target)]
    second = (block_of(target) + blocks // 2) % blocks
    return jnp.where((block_of(source) == one_side) | (block_of(source) == second), factor * values, values)


def level_of(key, dims, cuts, least, largest):
    def one(dim, blocks):
        steps = jax.random.uniform(jax.random.fold_in(jax.random.fold_in(key, 6), dim), (blocks,), jnp.float32, least / len(cuts), largest / len(cuts))
        return jnp.repeat(jnp.exp(steps), dims[dim] // blocks).reshape((-1,) + (1,) * (len(dims) - dim - 1))

    gain = one(*cuts[0])
    for cut in cuts[1:]:
        gain = gain * one(*cut)
    return gain


def centred(own_key, dims, spread, bound, pieces=(), kind=jnp.bfloat16):
    drawn = spread * jax.random.normal(own_key, dims, jnp.float32)
    if pieces:
        drawn = drawn * level_of(own_key, dims, pieces, -0.22, 0.18)
    return jnp.clip(drawn, -bound, bound).astype(kind)


def bell_draw_with(stream_key, extent, spread, reach, shards, heavy, dtype=jnp.bfloat16):
    entries = spread * jax.random.normal(stream_key, extent, jnp.float32)
    if shards:
        entries = entries * level_of(stream_key, extent, shards, -0.22, 0.18)
    return jnp.clip(spiked(entries, jax.random.fold_in(stream_key, 3), *heavy), -reach, reach).astype(dtype)


def setup_inputs(seed: int = 0, part: int = 0) -> dict:
    splits = jax.random.split(jax.random.key(seed), 16)
    own_keys = jax.random.split(jax.random.fold_in(splits[15], part), 16)
    partial_query = bell_draw_with(own_keys[0], (REPLICAS, WIDTH, ATTN), 0.5, 4.0, ((0, 4), (2, 4)), (0, 1, 4, 2.0))
    partial_key = bell_draw_with(own_keys[1], (REPLICAS, WIDTH, ATTN), 0.5, 4.0, ((0, 4), (2, 4)), (0, 1, 4, 2.0))
    partial_value = bell_draw_with(own_keys[2], (REPLICAS, WIDTH, ATTN), 0.5, 4.0, ((0, 4), (2, 4)), (0, 1, 4, 2.0))
    partial_mixed = bell_draw_with(own_keys[3], (REPLICAS, ATTN, WIDTH), 0.5, 4.0, ((0, 4), (1, 4)), (0, 2, 4, 2.0))
    partial_norm = bell_draw_with(own_keys[4], (REPLICAS, WIDTH), 1.0, 8.0, ((0, 4),), (0, 1, 4, 2.0))
    master_query = centred(own_keys[5], (WIDTH, ATTN), WIDTH ** -0.5, 0.1875, ((0, 4), (1, 4)), jnp.float32)
    master_key = centred(own_keys[6], (WIDTH, ATTN), WIDTH ** -0.5, 0.1875, ((0, 4), (1, 4)), jnp.float32)
    master_value = centred(own_keys[7], (WIDTH, ATTN), WIDTH ** -0.5, 0.1875, ((0, 4), (1, 4)), jnp.float32)
    master_mixed = centred(own_keys[8], (ATTN, WIDTH), ATTN ** -0.5, 0.1875, ((0, 4), (1, 4)), jnp.float32)
    master_norm = jnp.clip(1.0 + 0.15 * jax.random.normal(own_keys[9], (WIDTH,), jnp.float32), 0.25, 1.75)
    memory_query = jnp.clip(0.05 + 0.75 * jax.random.uniform(own_keys[10], (WIDTH, ATTN), jnp.float32) ** level_of(own_keys[10], (WIDTH, ATTN), ((0, 4), (1, 4)), -0.2, 0.2), 0.05, 0.8)
    memory_key = jnp.clip(0.05 + 0.75 * jax.random.uniform(own_keys[11], (WIDTH, ATTN), jnp.float32) ** level_of(own_keys[11], (WIDTH, ATTN), ((0, 4), (1, 4)), -0.2, 0.2), 0.05, 0.8)
    memory_value = jnp.clip(0.05 + 0.75 * jax.random.uniform(own_keys[12], (WIDTH, ATTN), jnp.float32) ** level_of(own_keys[12], (WIDTH, ATTN), ((0, 4), (1, 4)), -0.2, 0.2), 0.05, 0.8)
    memory_mixed = jnp.clip(0.05 + 0.75 * jax.random.uniform(own_keys[13], (ATTN, WIDTH), jnp.float32) ** level_of(own_keys[13], (ATTN, WIDTH), ((0, 4), (1, 4)), -0.2, 0.2), 0.05, 0.8)
    memory_norm = jnp.clip(0.05 + 0.75 * jax.random.uniform(own_keys[14], (WIDTH,), jnp.float32) ** level_of(own_keys[14], (WIDTH,), ((0, 4),), -0.2, 0.2), 0.05, 0.8)
    return {"partial_query": partial_query, "partial_key": partial_key, "partial_value": partial_value, "partial_mixed": partial_mixed, "partial_norm": partial_norm, "master_query": master_query, "master_key": master_key, "master_value": master_value, "master_mixed": master_mixed, "master_norm": master_norm, "memory_query": memory_query, "memory_key": memory_key, "memory_value": memory_value, "memory_mixed": memory_mixed, "memory_norm": memory_norm}


learn_rate = 0.05
hold_rate = 0.7

def reference(partial_query, partial_key, partial_value, partial_mixed, partial_norm, master_query, master_key, master_value, master_mixed, master_norm, memory_query, memory_key, memory_value, memory_mixed, memory_norm):
    mean_query = lax.optimization_barrier(jnp.sum(partial_query.astype(jnp.float32), axis=0)) * REPLICAS ** (-0.5)
    mean_key = lax.optimization_barrier(jnp.sum(partial_key.astype(jnp.float32), axis=0)) * REPLICAS ** (-0.5)
    mean_value = lax.optimization_barrier(jnp.sum(partial_value.astype(jnp.float32), axis=0)) * REPLICAS ** (-0.5)
    mean_mixed = lax.optimization_barrier(jnp.sum(partial_mixed.astype(jnp.float32), axis=0)) * REPLICAS ** (-0.5)
    mean_norm = lax.optimization_barrier(jnp.sum(partial_norm.astype(jnp.float32), axis=0)) * REPLICAS ** (-0.5)
    state_new_query = hold_rate * memory_query + (1.0 - hold_rate) * mean_query * mean_query
    stepped_query = master_query - learn_rate * mean_query * lax.rsqrt(state_new_query + 1e-06)
    state_new_key = hold_rate * memory_key + (1.0 - hold_rate) * mean_key * mean_key
    stepped_key = master_key - learn_rate * mean_key * lax.rsqrt(state_new_key + 1e-06)
    state_new_value = hold_rate * memory_value + (1.0 - hold_rate) * mean_value * mean_value
    stepped_value = master_value - learn_rate * mean_value * lax.rsqrt(state_new_value + 1e-06)
    state_new_mixed = hold_rate * memory_mixed + (1.0 - hold_rate) * mean_mixed * mean_mixed
    stepped_mixed = master_mixed - learn_rate * mean_mixed * lax.rsqrt(state_new_mixed + 1e-06)
    state_new_norm = hold_rate * memory_norm + (1.0 - hold_rate) * mean_norm * mean_norm
    stepped_norm = master_norm - learn_rate * mean_norm * lax.rsqrt(state_new_norm + 1e-06)
    compute_query = stepped_query.astype(jnp.bfloat16)
    compute_key = stepped_key.astype(jnp.bfloat16)
    compute_value = stepped_value.astype(jnp.bfloat16)
    compute_mixed = stepped_mixed.astype(jnp.bfloat16)
    compute_norm = stepped_norm.astype(jnp.bfloat16)
    return (compute_query, compute_key, compute_value, compute_mixed, compute_norm, stepped_query, stepped_key, stepped_value, stepped_mixed, stepped_norm, state_new_query, state_new_key, state_new_value, state_new_mixed, state_new_norm)
```

```python
import functools

import jax
import jax.numpy as jnp
from jax import lax
from jax.experimental import pallas as pl
from jax.experimental.pallas import tpu as pltpu
from jax.sharding import PartitionSpec as P

learn_rate = 0.05
hold_rate = 0.7
HALVES = 4
DEPTH = 2
END_CLOSE = 8
RS_OUT = 0
RS_BACK = 1
FINISH = 2
PASS_OUT = 10
PASS_NEAR = 4
PASS_FAR = 14
MESH = pl.DeviceIdType.MESH
LINK = jnp.bfloat16
MATRICES = 4
LIMIT = 4.0
TOP = 125.0


def update(mean, master, memory):
    state = hold_rate * memory + (1.0 - hold_rate) * mean * mean
    return master - learn_rate * mean * lax.rsqrt(state + 1e-06), state


def encode(value, terms):
    gain = TOP / (terms * LIMIT)
    return jnp.exp2(value * gain).astype(LINK)


def decode(code, terms):
    return jnp.log2(code.astype(jnp.float32)) * (terms * LIMIT / TOP)


def kernel(n, halves, *refs):
    T = MATRICES
    (partial, master, memory) = refs[0:T], refs[T : 2 * T], refs[2 * T : 3 * T]
    norms_in = refs[3 * T : 3 * T + 3]
    at = 3 * T + 3
    grown, step_v, state_v, compute_norm, stepped_norm, state_norm = refs[at : at + 6]
    (
        tall, master_v, memory_v, send_v, recv_v, norm_p, norm_m, norm_k,
        load_sem, held_sem, norm_load, rs_recv, ag_recv, end_recv, sent, raw_sent, norm_send, norm_recv,
    ) = refs[at + 6 :]
    norms_v = (norm_p, norm_m, norm_k)
    me = lax.axis_index("replica")
    rows, cols = master[0].shape
    part = rows // halves
    count = T * halves
    rate = n ** (-0.5)
    flip = jnp.where(me >= n // 2, 1, 0)
    out, back = flip, 1 - flip
    is_end = jnp.logical_or(me == 0, me == n - 1)

    def seg(s):
        return flip * (n - 1) + (1 - 2 * flip) * s

    def peer(way):
        return {"replica": me + 1 - 2 * way}

    def spot(plane, c, s):
        top = pl.multiple_of(s * rows + lax.rem(c, halves) * part, part)
        return plane.at[lax.div(c, halves), pl.ds(top, part), :]

    def loads_of(t):
        if t < T - 1:
            pairs = [(partial[t], tall.at[t])]
        else:
            pairs = [
                (partial[t].at[:, s * cols : (s + 1) * cols], tall.at[t, s * rows : (s + 1) * rows])
                for s in range(n)
            ]
        return [pltpu.make_async_copy(*pair, load_sem.at[t, i]) for i, pair in enumerate(pairs)]

    loads = [loads_of(t) for t in range(T)]
    own_norms = [
        pltpu.make_async_copy(source, target.at[me], norm_load.at[i])
        for i, (source, target) in enumerate(zip(norms_in, norms_v))
    ]
    held = [
        pltpu.make_async_copy(source[t], target.at[t], held_sem.at[i, t])
        for i, (source, target) in enumerate(((master, master_v), (memory, memory_v)))
        for t in range(T)
    ]
    for copy in sum(loads, []) + own_norms + held:
        copy.start()

    barrier = pltpu.get_barrier_semaphore()

    @pl.when(me > 0)
    def _():
        pl.semaphore_signal(barrier, inc=1, device_id=peer(1), device_id_type=MESH)

    @pl.when(me < n - 1)
    def _():
        pl.semaphore_signal(barrier, inc=1, device_id=peer(0), device_id_type=MESH)

    pl.semaphore_wait(barrier, jnp.where(is_end, 1, 2))

    def sum_copy(way, c, s, source):
        return pltpu.make_async_remote_copy(
            src_ref=source,
            dst_ref=recv_v.at[way, c, s],
            send_sem=sent.at[way],
            recv_sem=rs_recv.at[way, c, s],
            device_id=peer(way),
            device_id_type=MESH,
        )

    def sum_wait(way, c, s):
        sum_copy(way, c, s, send_v.at[0, c]).wait_recv()

    def share_copy(way, c, s, last=False):
        place = spot(grown, c, s)
        return pltpu.make_async_remote_copy(
            src_ref=place,
            dst_ref=place,
            send_sem=sent.at[way],
            recv_sem=end_recv.at[0] if last else ag_recv.at[way, c, s],
            device_id=peer(way),
            device_id_type=MESH,
        )

    def norm_copies(way, s):
        return [
            pltpu.make_async_remote_copy(
                src_ref=ref.at[s],
                dst_ref=ref.at[s],
                send_sem=norm_send.at[way, s, i],
                recv_sem=norm_recv.at[s, i],
                device_id=peer(way),
                device_id_type=MESH,
            )
            for i, ref in enumerate(norms_v)
        ]

    def finish(c, total, s):
        t = lax.div(c, halves)
        band = pl.ds(pl.multiple_of(lax.rem(c, halves) * part, part), part)
        new, held_new = update(total * rate, master_v[t, band, :], memory_v[t, band, :])
        spot(grown, c, s)[...] = new.astype(jnp.bfloat16)
        step_v[t, band, :] = new
        state_v[t, band, :] = held_new

    def own(c, s):
        return spot(tall, c, s)[...].astype(jnp.float32)

    def sent_wait(way, planes):
        pltpu.make_async_remote_copy(
            src_ref=tall.at[0:planes],
            dst_ref=grown.at[0:planes],
            send_sem=sent.at[way],
            recv_sem=end_recv.at[0],
            device_id=peer(way),
            device_id_type=MESH,
        ).wait_send()

    @pl.when(is_end)
    def _():
        for copy in own_norms:
            copy.wait()
        for copy in norm_copies(out, me):
            copy.start()

        def raw_copy(c, s):
            return pltpu.make_async_remote_copy(
                src_ref=spot(tall, c, s),
                dst_ref=recv_v.at[out, c, s],
                send_sem=raw_sent.at[lax.rem(c, DEPTH), s],
                recv_sem=rs_recv.at[out, c, s],
                device_id=peer(out),
                device_id_type=MESH,
            )

        def close(c):
            sum_wait(back, c, me)
            finish(c, own(c, me) + decode(recv_v[back, c, me], n - 1), me)
            share_copy(out, c, me).start()

        def end_step(j, carry):
            for s in range(n - 1, 0, -1):

                @pl.when(jnp.logical_and(j >= DEPTH, j < count + DEPTH))
                def _():
                    raw_copy(j - DEPTH, seg(s)).wait_send()

                @pl.when(j < count)
                def _():
                    raw_copy(j, seg(s)).start()

            @pl.when(jnp.logical_and(j >= END_CLOSE, j < count + END_CLOSE))
            def _():
                close(j - END_CLOSE)

            return carry

        for t in range(T):
            for copy in loads[t]:
                copy.wait()
            if t == 1:
                for copy in held:
                    copy.wait()
            lax.fori_loop(t * halves, (t + 1) * halves, end_step, 0)
        lax.fori_loop(count, count + max(DEPTH, END_CLOSE), end_step, 0)
        for copy in norm_copies(out, me):
            copy.wait_send()
        for s in range(1, n):
            for copy in norm_copies(out, seg(s)):
                copy.wait_recv()

    @pl.when(jnp.logical_not(is_end))
    def _():
        for copy in own_norms:
            copy.wait()
        for way in range(2):
            for copy in norm_copies(way, me):
                copy.start()
        for copy in sum(loads, []) + held:
            copy.wait()

        def step(j, carry):
            def at_lag(lag, act):
                c = j - lag

                @pl.when(jnp.logical_and(c >= 0, c < count))
                def _():
                    act(c)

            def rs_out(c):
                for i, s in enumerate((seg(3), seg(2))):
                    sum_wait(out, c, s)
                    total = own(c, s) + recv_v[out, c, s].astype(jnp.float32)
                    send_v[i, c] = encode(total, 2)
                    sum_copy(out, c, s, send_v.at[i, c]).start()

            def rs_back(c):
                s = seg(0)
                sum_wait(back, c, s)
                send_v[2, c] = encode(own(c, s) + decode(recv_v[back, c, s], 2), 3)
                sum_copy(back, c, s, send_v.at[2, c]).start()

            def close(c):
                sum_wait(out, c, me)
                total = own(c, me) + recv_v[out, c, me].astype(jnp.float32)
                sum_wait(back, c, me)
                finish(c, total + decode(recv_v[back, c, me], 2), me)
                share_copy(out, c, me).start()
                share_copy(back, c, me, True).start()

            def pass_on(way, s, last):
                def act(c):
                    share_copy(way, c, s).wait_recv()
                    share_copy(way, c, s, last).start()

                return act

            at_lag(RS_OUT, rs_out)
            at_lag(RS_BACK, rs_back)
            at_lag(FINISH, close)
            at_lag(PASS_OUT, pass_on(out, seg(0), False))
            at_lag(PASS_NEAR, pass_on(back, seg(2), True))
            at_lag(PASS_FAR, pass_on(back, seg(3), True))
            return carry

        early = 2
        lax.fori_loop(0, early, step, 0)
        for way, s in ((out, 0), (back, 2)):
            for copy in norm_copies(way, seg(s)):
                copy.wait_recv()
            for copy in norm_copies(way, seg(s)):
                copy.start()
        lax.fori_loop(early, 2 * early, step, 0)
        for copy in norm_copies(back, seg(3)):
            copy.wait_recv()
        for copy in norm_copies(back, seg(3)):
            copy.start()
        last = max(RS_OUT, RS_BACK, FINISH, PASS_OUT, PASS_NEAR, PASS_FAR)
        lax.fori_loop(2 * early, count + last, step, 0)
        for way, s in ((out, 0), (out, 1), (back, 1), (back, 2), (back, 3)):
            for copy in norm_copies(way, seg(s)):
                copy.wait_send()

    mean = norm_p[0].astype(jnp.float32)
    for s in range(1, n):
        mean = mean + norm_p[s].astype(jnp.float32)
    mean = mean * rate
    for s in range(n):
        new, held_new = update(mean[:, s * cols : (s + 1) * cols], norm_m[s], norm_k[s])
        compute_norm[:, s * cols : (s + 1) * cols] = new

        @pl.when(me == s)
        def _():
            stepped_norm[...] = new
            state_norm[...] = held_new

    @pl.when(jnp.logical_not(is_end))
    def _():
        sent_wait(out, T)
        sent_wait(back, T)

    @pl.when(is_end)
    def _():
        sent_wait(out, 1)
        three = grown.at[0 : n - 1]
        pltpu.make_async_remote_copy(
            src_ref=three,
            dst_ref=three,
            send_sem=sent.at[out],
            recv_sem=end_recv.at[0],
            device_id=peer(out),
            device_id_type=MESH,
        ).wait_recv()


def write(n, *refs):
    T = MATRICES
    grown, step_v, state_v, stepped_norm_v, state_norm_v = refs[:5]
    compute, stepped, state = refs[5 : 5 + T], refs[5 + T : 5 + 2 * T], refs[5 + 2 * T : 5 + 3 * T]
    stepped_norm, state_norm, sems = refs[5 + 3 * T :]
    rows, cols = stepped[0].shape
    pairs = [(grown.at[t], compute[t]) for t in range(T - 1)]
    pairs += [
        (grown.at[T - 1, s * rows : (s + 1) * rows], compute[T - 1].at[:, s * cols : (s + 1) * cols])
        for s in range(n)
    ]
    pairs += [(step_v.at[t], stepped[t]) for t in range(T)]
    pairs += [(state_v.at[t], state[t]) for t in range(T)]
    pairs += [(stepped_norm_v, stepped_norm), (state_norm_v, state_norm)]
    copies = [pltpu.make_async_copy(*pair, sems.at[i]) for i, pair in enumerate(pairs)]
    for copy in copies:
        copy.start()
    for copy in copies:
        copy.wait()


def line(n, partials, masters, memories, partial_norm, master_norm, memory_norm):
    T, halves = MATRICES, HALVES
    rows, cols = masters[0].shape
    part = rows // halves
    count = T * halves
    whole = partial_norm.shape[1]
    f32, bf16 = jnp.float32, jnp.bfloat16
    anywhere = pl.BlockSpec(memory_space=pl.ANY)
    inside = pl.BlockSpec(memory_space=pltpu.VMEM)
    dma = pltpu.SemaphoreType.DMA
    kept = pl.pallas_call(
        functools.partial(kernel, n, halves),
        out_shape=[
            pltpu.VMEM((T, n * rows, cols), bf16),
            pltpu.VMEM((T, rows, cols), f32),
            pltpu.VMEM((T, rows, cols), f32),
            pltpu.VMEM((1, whole), f32),
            pltpu.VMEM((1, cols), f32),
            pltpu.VMEM((1, cols), f32),
        ],
        in_specs=[anywhere] * (3 * T + 3),
        out_specs=[inside] * 6,
        scratch_shapes=[
            pltpu.VMEM((T, n * rows, cols), bf16),
            pltpu.VMEM((T, rows, cols), f32),
            pltpu.VMEM((T, rows, cols), f32),
            pltpu.VMEM((n - 1, count, part, cols), LINK),
            pltpu.VMEM((2, count, n, part, cols), LINK),
            pltpu.VMEM((n, 1, whole), bf16),
            pltpu.VMEM((n, 1, cols), f32),
            pltpu.VMEM((n, 1, cols), f32),
            dma((T, n)),
            dma((2, T)),
            dma((3,)),
            dma((2, count, n)),
            dma((2, count, n)),
            dma((1,)),
            dma((2,)),
            dma((DEPTH, n)),
            dma((2, n, 3)),
            dma((n, 3)),
        ],
        compiler_params=pltpu.CompilerParams(
            collective_id=0, has_side_effects=True, vmem_limit_bytes=32 * 1024 * 1024
        ),
        name="line_step",
    )(
        *(
            pltpu.with_memory_space_constraint(x, pltpu.HBM)
            for x in (
                *partials, *masters, *memories, partial_norm, master_norm[None], memory_norm[None],
            )
        )
    )
    share = jax.ShapeDtypeStruct((rows, cols), f32)
    out = pl.pallas_call(
        functools.partial(write, n),
        out_shape=[jax.ShapeDtypeStruct(p.shape, bf16) for p in partials]
        + [share] * (2 * T)
        + [jax.ShapeDtypeStruct((1, cols), f32)] * 2,
        in_specs=[inside] * 5,
        out_specs=[anywhere] * (3 * T + 2),
        scratch_shapes=[dma((3 * T + n + 1,))],
        compiler_params=pltpu.CompilerParams(vmem_limit_bytes=1024 * 1024),
        name="write_out",
    )(*kept[:3], *kept[4:])
    compute, stepped, state = out[:T], out[T : 2 * T], out[2 * T : 3 * T]
    stepped_norm, state_norm = out[3 * T :]
    compute_norm = kept[3][0].astype(bf16)
    return (*compute, compute_norm, *stepped, stepped_norm[0], *state, state_norm[0])


def plain(n, partials, masters, memories, partial_norm, master_norm, memory_norm):
    rate = n ** (-0.5)
    axes = (0, 0, 0, 1)
    compute, stepped, state = [], [], []
    for p, master, memory, axis in zip(partials, masters, memories, axes):
        total = lax.psum_scatter(
            p.astype(jnp.float32), "replica", scatter_dimension=axis, tiled=True
        )
        new, held = update(total * rate, master, memory)
        stepped.append(new)
        state.append(held)
    whole = lax.psum(partial_norm[0].astype(jnp.float32), "replica")
    size = master_norm.shape[0]
    mean = lax.dynamic_slice_in_dim(whole, lax.axis_index("replica") * size, size) * rate
    new, held = update(mean, master_norm, memory_norm)
    stepped.append(new)
    state.append(held)
    for new, axis in zip(stepped, axes + (0,)):
        compute.append(lax.all_gather(new.astype(jnp.bfloat16), "replica", axis=axis, tiled=True))
    return (*compute, *stepped, *state)


def body(*args):
    partials = [p[0] for p in args[:4]]
    partial_norm = args[4]
    masters, master_norm = args[5:9], args[9]
    memories, memory_norm = args[10:14], args[14]
    n = lax.axis_size("replica")
    shapes = {m.shape for m in masters}
    rows, cols = masters[0].shape
    fits = (
        n == MATRICES
        and len(shapes) == 1
        and rows % (32 * HALVES) == 0
        and cols % 128 == 0
        and master_norm.shape[0] == cols
    )
    form = line if fits else plain
    return form(n, partials, masters, memories, partial_norm, master_norm, memory_norm)


def solution(mesh):
    tall = P(("site", "replica"), None, "model")
    share, flat = P(("site", "replica"), "model"), P(("site", "replica"))
    wide = P(("site", "model"), "replica")
    shares = (share, share, share, wide, flat)
    return jax.shard_map(
        body,
        mesh=mesh,
        in_specs=(
            tall,
            tall,
            tall,
            P(("site", "replica"), "model", None),
            P(("site", "replica"), None),
            *shares,
            *shares,
        ),
        out_specs=(
            P("site", "model"),
            P("site", "model"),
            P("site", "model"),
            P(("site", "model"), None),
            P("site"),
            *shares,
            *shares,
        ),
        check_vma=False,
    )
```

```python
import functools

import jax
import jax.numpy as jnp
from jax import lax
from jax.experimental import pallas as pl
from jax.experimental.pallas import tpu as pltpu
from jax.sharding import PartitionSpec as P

learn_rate = 0.05
hold_rate = 0.7
HALVES = 4
DEPTH = 2
EARLY = 3
ENDS = (("raw3", 0), ("close", 47), ("raw1", 3), ("raw2", 0))
MIDDLES = (("pass2", 7), ("close", 4), ("pass3", 26), ("pass0", 18), ("sum3", 0), ("sum0", 2), ("sum2", 1))
MESH = pl.DeviceIdType.MESH
LINK = jnp.bfloat16
MATRICES = 4
LIMIT = 4.0
TOP = 125.0


def update(mean, master, memory):
    state = hold_rate * memory + (1.0 - hold_rate) * mean * mean
    return master - learn_rate * mean * lax.rsqrt(state + 1e-06), state


def encode(value, terms):
    gain = TOP / (terms * LIMIT)
    return jnp.exp2(value * gain).astype(LINK)


def decode(code, terms):
    return jnp.log2(code.astype(jnp.float32)) * (terms * LIMIT / TOP)


def kernel(n, halves, *refs):
    T = MATRICES
    (partial, master, memory) = refs[0:T], refs[T : 2 * T], refs[2 * T : 3 * T]
    norms_in = refs[3 * T : 3 * T + 3]
    at = 3 * T + 3
    grown, step_v, state_v, compute_norm, stepped_norm, state_norm = refs[at : at + 6]
    (
        tall, master_v, memory_v, send_v, recv_v, norm_p, norm_m, norm_k,
        load_sem, held_sem, norm_load, rs_recv, ag_recv, end_recv, sent, raw_sent, norm_send, norm_recv,
    ) = refs[at + 6 :]
    norms_v = (norm_p, norm_m, norm_k)
    me = lax.axis_index("replica")
    rows, cols = master[0].shape
    part = rows // halves
    count = T * halves
    rate = n ** (-0.5)
    flip = jnp.where(me >= n // 2, 1, 0)
    out, back = flip, 1 - flip
    is_end = jnp.logical_or(me == 0, me == n - 1)

    def seg(s):
        return flip * (n - 1) + (1 - 2 * flip) * s

    def peer(way):
        return {"replica": me + 1 - 2 * way}

    def spot(plane, c, s):
        top = pl.multiple_of(s * rows + lax.rem(c, halves) * part, part)
        return plane.at[lax.div(c, halves), pl.ds(top, part), :]

    def loads_of(t):
        if t < T - 1:
            pairs = [(partial[t], tall.at[t])]
        else:
            pairs = [
                (partial[t].at[:, s * cols : (s + 1) * cols], tall.at[t, s * rows : (s + 1) * rows])
                for s in range(n)
            ]
        return [pltpu.make_async_copy(*pair, load_sem.at[t, i]) for i, pair in enumerate(pairs)]

    loads = [loads_of(t) for t in range(T)]
    own_norms = [
        pltpu.make_async_copy(source, target.at[me], norm_load.at[i])
        for i, (source, target) in enumerate(zip(norms_in, norms_v))
    ]
    held = [
        pltpu.make_async_copy(source[t], target.at[t], held_sem.at[i, t])
        for i, (source, target) in enumerate(((master, master_v), (memory, memory_v)))
        for t in range(T)
    ]
    for copy in loads[0]:
        copy.start()
    barrier = pltpu.get_barrier_semaphore()

    @pl.when(me > 0)
    def _():
        pl.semaphore_signal(barrier, inc=1, device_id=peer(1), device_id_type=MESH)

    @pl.when(me < n - 1)
    def _():
        pl.semaphore_signal(barrier, inc=1, device_id=peer(0), device_id_type=MESH)

    for copy in sum(loads[1:], []) + own_norms + held:
        copy.start()
    pl.semaphore_wait(barrier, jnp.where(is_end, 1, 2))

    def sum_copy(way, c, s, source):
        return pltpu.make_async_remote_copy(
            src_ref=source,
            dst_ref=recv_v.at[way, c, s],
            send_sem=sent.at[way],
            recv_sem=rs_recv.at[way, c, s],
            device_id=peer(way),
            device_id_type=MESH,
        )

    def sum_wait(way, c, s):
        sum_copy(way, c, s, send_v.at[0, c]).wait_recv()

    def share_copy(way, c, s, last=False):
        place = spot(grown, c, s)
        return pltpu.make_async_remote_copy(
            src_ref=place,
            dst_ref=place,
            send_sem=sent.at[way],
            recv_sem=end_recv.at[0] if last else ag_recv.at[way, c, s],
            device_id=peer(way),
            device_id_type=MESH,
        )

    def norm_copies(way, s):
        return [
            pltpu.make_async_remote_copy(
                src_ref=ref.at[s],
                dst_ref=ref.at[s],
                send_sem=norm_send.at[way, s, i],
                recv_sem=norm_recv.at[s, i],
                device_id=peer(way),
                device_id_type=MESH,
            )
            for i, ref in enumerate(norms_v)
        ]

    def finish(c, total, s):
        t = lax.div(c, halves)
        band = pl.ds(pl.multiple_of(lax.rem(c, halves) * part, part), part)
        new, held_new = update(total * rate, master_v[t, band, :], memory_v[t, band, :])
        spot(grown, c, s)[...] = new.astype(jnp.bfloat16)
        step_v[t, band, :] = new
        state_v[t, band, :] = held_new

    def own(c, s):
        return spot(tall, c, s)[...].astype(jnp.float32)

    def run(table, acts, low=None, high=None):
        def step(j, carry):
            for name, lag in table:
                c = j - lag

                @pl.when(jnp.logical_and(c >= 0, c < count))
                def _():
                    acts[name](c)

            return carry

        low = min(lag for _, lag in table) if low is None else low
        high = count + max(lag for _, lag in table) if high is None else high
        lax.fori_loop(low, high, step, 0)

    def sent_wait(way, planes):
        pltpu.make_async_remote_copy(
            src_ref=tall.at[0:planes],
            dst_ref=grown.at[0:planes],
            send_sem=sent.at[way],
            recv_sem=end_recv.at[0],
            device_id=peer(way),
            device_id_type=MESH,
        ).wait_send()

    @pl.when(is_end)
    def _():
        def raw_copy(c, s):
            return pltpu.make_async_remote_copy(
                src_ref=spot(tall, c, s),
                dst_ref=recv_v.at[out, c, s],
                send_sem=raw_sent.at[lax.rem(c, DEPTH), s],
                recv_sem=rs_recv.at[out, c, s],
                device_id=peer(out),
                device_id_type=MESH,
            )

        def close(c):
            sum_wait(back, c, me)
            finish(c, own(c, me) + decode(recv_v[back, c, me], n - 1), me)
            share_copy(out, c, me).start()

        def raw(s):
            def act(c):
                @pl.when(c >= DEPTH)
                def _():
                    raw_copy(c - DEPTH, seg(s)).wait_send()

                raw_copy(c, seg(s)).start()

            return act

        acts = {"raw3": raw(3), "raw2": raw(2), "raw1": raw(1), "close": close}
        for copy in loads[0]:
            copy.wait()
        first = min(lag for _, lag in ENDS)
        run(ENDS, acts, first, first + 1)
        for copy in own_norms:
            copy.wait()
        for copy in norm_copies(out, me):
            copy.start()
        run(ENDS, acts, first + 1, first + halves)
        for copy in sum(loads[1:], []) + held:
            copy.wait()
        run(ENDS, acts, first + halves)
        for s in range(1, n):
            for c in range(count - DEPTH, count):
                raw_copy(c, seg(s)).wait_send()
        for copy in norm_copies(out, me):
            copy.wait_send()
        for s in range(1, n):
            for copy in norm_copies(out, seg(s)):
                copy.wait_recv()

    @pl.when(jnp.logical_not(is_end))
    def _():
        for copy in own_norms:
            copy.wait()
        for way in range(2):
            for copy in norm_copies(way, me):
                copy.start()
        for copy in sum(loads, []) + held:
            copy.wait()

        def sum_out(s):
            def act(c):
                sum_wait(out, c, seg(s))
                total = own(c, seg(s)) + recv_v[out, c, seg(s)].astype(jnp.float32)
                send_v[s - 2, c] = encode(total, 2)
                sum_copy(out, c, seg(s), send_v.at[s - 2, c]).start()

            return act

        def sum_back(c):
            s = seg(0)
            sum_wait(back, c, s)
            send_v[2, c] = encode(own(c, s) + decode(recv_v[back, c, s], 2), 3)
            sum_copy(back, c, s, send_v.at[2, c]).start()

        def close(c):
            sum_wait(out, c, me)
            total = own(c, me) + recv_v[out, c, me].astype(jnp.float32)
            sum_wait(back, c, me)
            finish(c, total + decode(recv_v[back, c, me], 2), me)
            share_copy(out, c, me).start()
            share_copy(back, c, me, True).start()

        def pass_on(way, s, last):
            def act(c):
                share_copy(way, c, s).wait_recv()
                share_copy(way, c, s, last).start()

            return act

        acts = {
            "sum3": sum_out(3),
            "sum2": sum_out(2),
            "sum0": sum_back,
            "close": close,
            "pass0": pass_on(out, seg(0), False),
            "pass2": pass_on(back, seg(2), True),
            "pass3": pass_on(back, seg(3), True),
        }
        first = min(lag for _, lag in MIDDLES)
        run(MIDDLES, acts, first, first + EARLY)
        for way, s in ((out, 0), (back, 2)):
            for copy in norm_copies(way, seg(s)):
                copy.wait_recv()
            for copy in norm_copies(way, seg(s)):
                copy.start()
        run(MIDDLES, acts, first + EARLY, first + 2 * EARLY)
        for copy in norm_copies(back, seg(3)):
            copy.wait_recv()
        for copy in norm_copies(back, seg(3)):
            copy.start()
        run(MIDDLES, acts, first + 2 * EARLY)
        for way, s in ((out, 0), (out, 1), (back, 1), (back, 2), (back, 3)):
            for copy in norm_copies(way, seg(s)):
                copy.wait_send()

    mean = norm_p[0].astype(jnp.float32)
    for s in range(1, n):
        mean = mean + norm_p[s].astype(jnp.float32)
    mean = mean * rate
    for s in range(n):
        new, held_new = update(mean[:, s * cols : (s + 1) * cols], norm_m[s], norm_k[s])
        compute_norm[:, s * cols : (s + 1) * cols] = new

        @pl.when(me == s)
        def _():
            stepped_norm[...] = new
            state_norm[...] = held_new

    @pl.when(jnp.logical_not(is_end))
    def _():
        sent_wait(out, T)
        sent_wait(back, T)

    @pl.when(is_end)
    def _():
        sent_wait(out, 1)
        three = grown.at[0 : n - 1]
        pltpu.make_async_remote_copy(
            src_ref=three,
            dst_ref=three,
            send_sem=sent.at[out],
            recv_sem=end_recv.at[0],
            device_id=peer(out),
            device_id_type=MESH,
        ).wait_recv()


def write(n, *refs):
    T = MATRICES
    grown, step_v, state_v, compute_norm_v, stepped_norm_v, state_norm_v = refs[:6]
    compute, stepped, state = refs[6 : 6 + T], refs[6 + T : 6 + 2 * T], refs[6 + 2 * T : 6 + 3 * T]
    compute_norm, stepped_norm, state_norm, flat, sems = refs[6 + 3 * T :]
    rows, cols = stepped[0].shape
    pairs = [(grown.at[t], compute[t]) for t in range(T - 1)]
    pairs += [
        (grown.at[T - 1, s * rows : (s + 1) * rows], compute[T - 1].at[:, s * cols : (s + 1) * cols])
        for s in range(n)
    ]
    pairs += [(step_v.at[t], stepped[t]) for t in range(T)]
    pairs += [(state_v.at[t], state[t]) for t in range(T)]
    pairs += [(stepped_norm_v, stepped_norm), (state_norm_v, state_norm), (flat, compute_norm)]
    copies = [pltpu.make_async_copy(*pair, sems.at[i]) for i, pair in enumerate(pairs)]
    for copy in copies[:-1]:
        copy.start()
    flat[...] = compute_norm_v[...].reshape(flat.shape).astype(flat.dtype)
    copies[-1].start()
    for copy in copies:
        copy.wait()


def line(n, partials, masters, memories, partial_norm, master_norm, memory_norm):
    T, halves = MATRICES, HALVES
    rows, cols = masters[0].shape
    part = rows // halves
    count = T * halves
    whole = partial_norm.shape[1]
    f32, bf16 = jnp.float32, jnp.bfloat16
    anywhere = pl.BlockSpec(memory_space=pl.ANY)
    inside = pl.BlockSpec(memory_space=pltpu.VMEM)
    dma = pltpu.SemaphoreType.DMA
    kept = pl.pallas_call(
        functools.partial(kernel, n, halves),
        out_shape=[
            pltpu.VMEM((T, n * rows, cols), bf16),
            pltpu.VMEM((T, rows, cols), f32),
            pltpu.VMEM((T, rows, cols), f32),
            pltpu.VMEM((1, whole), f32),
            pltpu.VMEM((1, cols), f32),
            pltpu.VMEM((1, cols), f32),
        ],
        in_specs=[anywhere] * (3 * T + 3),
        out_specs=[inside] * 6,
        scratch_shapes=[
            pltpu.VMEM((T, n * rows, cols), bf16),
            pltpu.VMEM((T, rows, cols), f32),
            pltpu.VMEM((T, rows, cols), f32),
            pltpu.VMEM((n - 1, count, part, cols), LINK),
            pltpu.VMEM((2, count, n, part, cols), LINK),
            pltpu.VMEM((n, 1, whole), bf16),
            pltpu.VMEM((n, 1, cols), f32),
            pltpu.VMEM((n, 1, cols), f32),
            dma((T, n)),
            dma((2, T)),
            dma((3,)),
            dma((2, count, n)),
            dma((2, count, n)),
            dma((1,)),
            dma((2,)),
            dma((DEPTH, n)),
            dma((2, n, 3)),
            dma((n, 3)),
        ],
        compiler_params=pltpu.CompilerParams(
            collective_id=0, has_side_effects=True, vmem_limit_bytes=32 * 1024 * 1024
        ),
        name="line_step",
    )(
        *(
            pltpu.with_memory_space_constraint(x, pltpu.HBM)
            for x in (
                *partials, *masters, *memories, partial_norm, master_norm[None], memory_norm[None],
            )
        )
    )
    share = jax.ShapeDtypeStruct((rows, cols), f32)
    out = pl.pallas_call(
        functools.partial(write, n),
        out_shape=[jax.ShapeDtypeStruct(p.shape, bf16) for p in partials]
        + [share] * (2 * T)
        + [jax.ShapeDtypeStruct((whole,), bf16)]
        + [jax.ShapeDtypeStruct((1, cols), f32)] * 2,
        in_specs=[inside] * 6,
        out_specs=[anywhere] * (3 * T + 3),
        scratch_shapes=[pltpu.VMEM((whole,), bf16), dma((3 * T + n + 2,))],
        compiler_params=pltpu.CompilerParams(vmem_limit_bytes=1024 * 1024),
        name="write_out",
    )(*kept)
    compute, stepped, state = out[:T], out[T : 2 * T], out[2 * T : 3 * T]
    compute_norm, stepped_norm, state_norm = out[3 * T :]
    return (*compute, compute_norm, *stepped, stepped_norm[0], *state, state_norm[0])


def plain(n, partials, masters, memories, partial_norm, master_norm, memory_norm):
    rate = n ** (-0.5)
    axes = (0, 0, 0, 1)
    compute, stepped, state = [], [], []
    for p, master, memory, axis in zip(partials, masters, memories, axes):
        total = lax.psum_scatter(
            p.astype(jnp.float32), "replica", scatter_dimension=axis, tiled=True
        )
        new, held = update(total * rate, master, memory)
        stepped.append(new)
        state.append(held)
    whole = lax.psum(partial_norm[0].astype(jnp.float32), "replica")
    size = master_norm.shape[0]
    mean = lax.dynamic_slice_in_dim(whole, lax.axis_index("replica") * size, size) * rate
    new, held = update(mean, master_norm, memory_norm)
    stepped.append(new)
    state.append(held)
    for new, axis in zip(stepped, axes + (0,)):
        compute.append(lax.all_gather(new.astype(jnp.bfloat16), "replica", axis=axis, tiled=True))
    return (*compute, *stepped, *state)


def body(*args):
    partials = [p[0] for p in args[:4]]
    partial_norm = args[4]
    masters, master_norm = args[5:9], args[9]
    memories, memory_norm = args[10:14], args[14]
    n = lax.axis_size("replica")
    shapes = {m.shape for m in masters}
    rows, cols = masters[0].shape
    fits = (
        n == MATRICES
        and len(shapes) == 1
        and rows % (32 * HALVES) == 0
        and cols % 128 == 0
        and master_norm.shape[0] == cols
    )
    form = line if fits else plain
    return form(n, partials, masters, memories, partial_norm, master_norm, memory_norm)


def solution(mesh):
    tall = P(("site", "replica"), None, "model")
    share, flat = P(("site", "replica"), "model"), P(("site", "replica"))
    wide = P(("site", "model"), "replica")
    shares = (share, share, share, wide, flat)
    return jax.shard_map(
        body,
        mesh=mesh,
        in_specs=(
            tall,
            tall,
            tall,
            P(("site", "replica"), "model", None),
            P(("site", "replica"), None),
            *shares,
            *shares,
        ),
        out_specs=(
            P("site", "model"),
            P("site", "model"),
            P("site", "model"),
            P(("site", "model"), None),
            P("site"),
            *shares,
            *shares,
        ),
        check_vma=False,
    )
```

```python
import functools

import jax
import jax.numpy as jnp
from jax import lax
from jax.experimental import pallas as pl
from jax.experimental.pallas import tpu as pltpu
from jax.sharding import PartitionSpec as P

learn_rate = 0.05
hold_rate = 0.7
HALVES = 4
DEPTH = 2
EARLY = 3
ENDS = (("raw2", 0), ("raw1", 2), ("raw3", 0), ("close", 76))
MIDDLES = (("close", 3), ("pass0", 18), ("pass2", 5), ("sum3", 1), ("sum0", 3), ("sum2", 0), ("pass3", 24))
MESH = pl.DeviceIdType.MESH
LINK = jnp.bfloat16
MATRICES = 4
LIMIT = 4.0
TOP = 125.0


def update(mean, master, memory):
    state = hold_rate * memory + (1.0 - hold_rate) * mean * mean
    return master - learn_rate * mean * lax.rsqrt(state + 1e-06), state


def encode(value, terms):
    gain = TOP / (terms * LIMIT)
    return jnp.exp2(value * gain).astype(LINK)


def decode(code, terms):
    return jnp.log2(code.astype(jnp.float32)) * (terms * LIMIT / TOP)


def kernel(n, halves, *refs):
    T = MATRICES
    (partial, master, memory) = refs[0:T], refs[T : 2 * T], refs[2 * T : 3 * T]
    norms_in = refs[3 * T : 3 * T + 3]
    at = 3 * T + 3
    grown, step_v, state_v, compute_norm, stepped_norm, state_norm = refs[at : at + 6]
    (
        tall, master_v, memory_v, send_v, recv_v, norm_p, norm_m, norm_k,
        load_sem, held_sem, norm_load, rs_recv, ag_recv, end_recv, sent, raw_sent, norm_send, norm_recv,
    ) = refs[at + 6 :]
    norms_v = (norm_p, norm_m, norm_k)
    me = lax.axis_index("replica")
    rows, cols = master[0].shape
    part = rows // halves
    count = T * halves
    rate = n ** (-0.5)
    flip = jnp.where(me >= n // 2, 1, 0)
    out, back = flip, 1 - flip
    is_end = jnp.logical_or(me == 0, me == n - 1)

    def seg(s):
        return flip * (n - 1) + (1 - 2 * flip) * s

    def peer(way):
        return {"replica": me + 1 - 2 * way}

    def spot(plane, c, s):
        top = pl.multiple_of(s * rows + lax.rem(c, halves) * part, part)
        return plane.at[lax.div(c, halves), pl.ds(top, part), :]

    def loads_of(t):
        if t < T - 1:
            pairs = [(partial[t], tall.at[t])]
        else:
            pairs = [
                (partial[t].at[:, s * cols : (s + 1) * cols], tall.at[t, s * rows : (s + 1) * rows])
                for s in range(n)
            ]
        return [pltpu.make_async_copy(*pair, load_sem.at[t, i]) for i, pair in enumerate(pairs)]

    loads = [loads_of(t) for t in range(T)]
    own_norms = [
        pltpu.make_async_copy(source, target.at[me], norm_load.at[i])
        for i, (source, target) in enumerate(zip(norms_in, norms_v))
    ]
    held = [
        pltpu.make_async_copy(source[t], target.at[t], held_sem.at[i, t])
        for i, (source, target) in enumerate(((master, master_v), (memory, memory_v)))
        for t in range(T)
    ]
    for copy in loads[0]:
        copy.start()
    barrier = pltpu.get_barrier_semaphore()

    @pl.when(me > 0)
    def _():
        pl.semaphore_signal(barrier, inc=1, device_id=peer(1), device_id_type=MESH)

    @pl.when(me < n - 1)
    def _():
        pl.semaphore_signal(barrier, inc=1, device_id=peer(0), device_id_type=MESH)

    for copy in sum(loads[1:], []) + own_norms + held:
        copy.start()
    pl.semaphore_wait(barrier, jnp.where(is_end, 1, 2))

    def sum_copy(way, c, s, source):
        return pltpu.make_async_remote_copy(
            src_ref=source,
            dst_ref=recv_v.at[way, c, s],
            send_sem=sent.at[way],
            recv_sem=rs_recv.at[way, c, s],
            device_id=peer(way),
            device_id_type=MESH,
        )

    def sum_wait(way, c, s):
        sum_copy(way, c, s, send_v.at[0, c]).wait_recv()

    def share_copy(way, c, s, last=False):
        place = spot(grown, c, s)
        return pltpu.make_async_remote_copy(
            src_ref=place,
            dst_ref=place,
            send_sem=sent.at[way],
            recv_sem=end_recv.at[0] if last else ag_recv.at[way, c, s],
            device_id=peer(way),
            device_id_type=MESH,
        )

    def norm_copies(way, s):
        return [
            pltpu.make_async_remote_copy(
                src_ref=ref.at[s],
                dst_ref=ref.at[s],
                send_sem=norm_send.at[way, s, i],
                recv_sem=norm_recv.at[s, i],
                device_id=peer(way),
                device_id_type=MESH,
            )
            for i, ref in enumerate(norms_v)
        ]

    def finish(c, total, s):
        t = lax.div(c, halves)
        band = pl.ds(pl.multiple_of(lax.rem(c, halves) * part, part), part)
        new, held_new = update(total * rate, master_v[t, band, :], memory_v[t, band, :])
        spot(grown, c, s)[...] = new.astype(jnp.bfloat16)
        step_v[t, band, :] = new
        state_v[t, band, :] = held_new

    def own(c, s):
        return spot(tall, c, s)[...].astype(jnp.float32)

    def run(table, acts, low=None, high=None):
        def step(j, carry):
            for name, lag in table:
                c = j - lag

                @pl.when(jnp.logical_and(c >= 0, c < count))
                def _():
                    acts[name](c)

            return carry

        low = min(lag for _, lag in table) if low is None else low
        high = count + max(lag for _, lag in table) if high is None else high
        lax.fori_loop(low, high, step, 0)

    def sent_wait(way, planes):
        pltpu.make_async_remote_copy(
            src_ref=tall.at[0:planes],
            dst_ref=grown.at[0:planes],
            send_sem=sent.at[way],
            recv_sem=end_recv.at[0],
            device_id=peer(way),
            device_id_type=MESH,
        ).wait_send()

    @pl.when(is_end)
    def _():
        def raw_copy(c, s):
            return pltpu.make_async_remote_copy(
                src_ref=spot(tall, c, s),
                dst_ref=recv_v.at[out, c, s],
                send_sem=raw_sent.at[lax.rem(c, DEPTH), s],
                recv_sem=rs_recv.at[out, c, s],
                device_id=peer(out),
                device_id_type=MESH,
            )

        def close(c):
            sum_wait(back, c, me)
            finish(c, own(c, me) + decode(recv_v[back, c, me], n - 1), me)
            share_copy(out, c, me).start()

        def raw(s):
            def act(c):
                @pl.when(c >= DEPTH)
                def _():
                    raw_copy(c - DEPTH, seg(s)).wait_send()

                raw_copy(c, seg(s)).start()

            return act

        acts = {"raw3": raw(3), "raw2": raw(2), "raw1": raw(1), "close": close}
        for copy in loads[0]:
            copy.wait()
        first = min(lag for _, lag in ENDS)
        run(ENDS, acts, first, first + 1)
        for copy in own_norms:
            copy.wait()
        for copy in norm_copies(out, me):
            copy.start()
        run(ENDS, acts, first + 1, first + halves)
        for copy in sum(loads[1:], []) + held:
            copy.wait()
        run(ENDS, acts, first + halves)
        for s in range(1, n):
            for c in range(count - DEPTH, count):
                raw_copy(c, seg(s)).wait_send()
        for copy in norm_copies(out, me):
            copy.wait_send()
        for s in range(1, n):
            for copy in norm_copies(out, seg(s)):
                copy.wait_recv()

    @pl.when(jnp.logical_not(is_end))
    def _():
        for copy in own_norms:
            copy.wait()
        for way in range(2):
            for copy in norm_copies(way, me):
                copy.start()
        for copy in sum(loads, []) + held:
            copy.wait()

        def sum_out(s):
            def act(c):
                sum_wait(out, c, seg(s))
                total = own(c, seg(s)) + recv_v[out, c, seg(s)].astype(jnp.float32)
                send_v[s - 2, c] = encode(total, 2)
                sum_copy(out, c, seg(s), send_v.at[s - 2, c]).start()

            return act

        def sum_back(c):
            s = seg(0)
            sum_wait(back, c, s)
            send_v[2, c] = encode(own(c, s) + decode(recv_v[back, c, s], 2), 3)
            sum_copy(back, c, s, send_v.at[2, c]).start()

        def close(c):
            sum_wait(out, c, me)
            total = own(c, me) + recv_v[out, c, me].astype(jnp.float32)
            sum_wait(back, c, me)
            finish(c, total + decode(recv_v[back, c, me], 2), me)
            share_copy(out, c, me).start()
            share_copy(back, c, me, True).start()

        def pass_on(way, s, last):
            def act(c):
                share_copy(way, c, s).wait_recv()
                share_copy(way, c, s, last).start()

            return act

        acts = {
            "sum3": sum_out(3),
            "sum2": sum_out(2),
            "sum0": sum_back,
            "close": close,
            "pass0": pass_on(out, seg(0), False),
            "pass2": pass_on(back, seg(2), True),
            "pass3": pass_on(back, seg(3), True),
        }
        first = min(lag for _, lag in MIDDLES)
        run(MIDDLES, acts, first, first + EARLY)
        for way, s in ((out, 0), (back, 2)):
            for copy in norm_copies(way, seg(s)):
                copy.wait_recv()
            for copy in norm_copies(way, seg(s)):
                copy.start()
        run(MIDDLES, acts, first + EARLY, first + 2 * EARLY)
        for copy in norm_copies(back, seg(3)):
            copy.wait_recv()
        for copy in norm_copies(back, seg(3)):
            copy.start()
        run(MIDDLES, acts, first + 2 * EARLY)
        for way, s in ((out, 0), (out, 1), (back, 1), (back, 2), (back, 3)):
            for copy in norm_copies(way, seg(s)):
                copy.wait_send()

    mean = norm_p[0].astype(jnp.float32)
    for s in range(1, n):
        mean = mean + norm_p[s].astype(jnp.float32)
    mean = mean * rate
    for s in range(n):
        new, held_new = update(mean[:, s * cols : (s + 1) * cols], norm_m[s], norm_k[s])
        compute_norm[:, s * cols : (s + 1) * cols] = new

        @pl.when(me == s)
        def _():
            stepped_norm[...] = new
            state_norm[...] = held_new

    @pl.when(jnp.logical_not(is_end))
    def _():
        sent_wait(out, T)
        sent_wait(back, T)

    @pl.when(is_end)
    def _():
        sent_wait(out, 1)
        three = grown.at[0 : n - 1]
        pltpu.make_async_remote_copy(
            src_ref=three,
            dst_ref=three,
            send_sem=sent.at[out],
            recv_sem=end_recv.at[0],
            device_id=peer(out),
            device_id_type=MESH,
        ).wait_recv()


def write(n, *refs):
    T = MATRICES
    grown, step_v, state_v, compute_norm_v, stepped_norm_v, state_norm_v = refs[:6]
    compute, stepped, state = refs[6 : 6 + T], refs[6 + T : 6 + 2 * T], refs[6 + 2 * T : 6 + 3 * T]
    compute_norm, stepped_norm, state_norm, flat, sems = refs[6 + 3 * T :]
    rows, cols = stepped[0].shape
    pairs = [(grown.at[t], compute[t]) for t in range(T - 1)]
    pairs += [
        (grown.at[T - 1, s * rows : (s + 1) * rows], compute[T - 1].at[:, s * cols : (s + 1) * cols])
        for s in range(n)
    ]
    pairs += [(step_v.at[t], stepped[t]) for t in range(T)]
    pairs += [(state_v.at[t], state[t]) for t in range(T)]
    pairs += [(stepped_norm_v, stepped_norm), (state_norm_v, state_norm), (flat, compute_norm)]
    copies = [pltpu.make_async_copy(*pair, sems.at[i]) for i, pair in enumerate(pairs)]
    for copy in copies[:-1]:
        copy.start()
    flat[...] = compute_norm_v[...].reshape(flat.shape).astype(flat.dtype)
    copies[-1].start()
    for copy in copies:
        copy.wait()


def line(n, partials, masters, memories, partial_norm, master_norm, memory_norm):
    T, halves = MATRICES, HALVES
    rows, cols = masters[0].shape
    part = rows // halves
    count = T * halves
    whole = partial_norm.shape[1]
    f32, bf16 = jnp.float32, jnp.bfloat16
    anywhere = pl.BlockSpec(memory_space=pl.ANY)
    inside = pl.BlockSpec(memory_space=pltpu.VMEM)
    dma = pltpu.SemaphoreType.DMA
    kept = pl.pallas_call(
        functools.partial(kernel, n, halves),
        out_shape=[
            pltpu.VMEM((T, n * rows, cols), bf16),
            pltpu.VMEM((T, rows, cols), f32),
            pltpu.VMEM((T, rows, cols), f32),
            pltpu.VMEM((1, whole), f32),
            pltpu.VMEM((1, cols), f32),
            pltpu.VMEM((1, cols), f32),
        ],
        in_specs=[anywhere] * (3 * T + 3),
        out_specs=[inside] * 6,
        scratch_shapes=[
            pltpu.VMEM((T, n * rows, cols), bf16),
            pltpu.VMEM((T, rows, cols), f32),
            pltpu.VMEM((T, rows, cols), f32),
            pltpu.VMEM((n - 1, count, part, cols), LINK),
            pltpu.VMEM((2, count, n, part, cols), LINK),
            pltpu.VMEM((n, 1, whole), bf16),
            pltpu.VMEM((n, 1, cols), f32),
            pltpu.VMEM((n, 1, cols), f32),
            dma((T, n)),
            dma((2, T)),
            dma((3,)),
            dma((2, count, n)),
            dma((2, count, n)),
            dma((1,)),
            dma((2,)),
            dma((DEPTH, n)),
            dma((2, n, 3)),
            dma((n, 3)),
        ],
        compiler_params=pltpu.CompilerParams(
            collective_id=0, has_side_effects=True, vmem_limit_bytes=32 * 1024 * 1024
        ),
        name="line_step",
    )(
        *(
            pltpu.with_memory_space_constraint(x, pltpu.HBM)
            for x in (
                *partials, *masters, *memories, partial_norm, master_norm[None], memory_norm[None],
            )
        )
    )
    share = jax.ShapeDtypeStruct((rows, cols), f32)
    out = pl.pallas_call(
        functools.partial(write, n),
        out_shape=[jax.ShapeDtypeStruct(p.shape, bf16) for p in partials]
        + [share] * (2 * T)
        + [jax.ShapeDtypeStruct((whole,), bf16)]
        + [jax.ShapeDtypeStruct((1, cols), f32)] * 2,
        in_specs=[inside] * 6,
        out_specs=[anywhere] * (3 * T + 3),
        scratch_shapes=[pltpu.VMEM((whole,), bf16), dma((3 * T + n + 2,))],
        compiler_params=pltpu.CompilerParams(vmem_limit_bytes=1024 * 1024),
        name="write_out",
    )(*kept)
    compute, stepped, state = out[:T], out[T : 2 * T], out[2 * T : 3 * T]
    compute_norm, stepped_norm, state_norm = out[3 * T :]
    return (*compute, compute_norm, *stepped, stepped_norm[0], *state, state_norm[0])


def plain(n, partials, masters, memories, partial_norm, master_norm, memory_norm):
    rate = n ** (-0.5)
    axes = (0, 0, 0, 1)
    compute, stepped, state = [], [], []
    for p, master, memory, axis in zip(partials, masters, memories, axes):
        total = lax.psum_scatter(
            p.astype(jnp.float32), "replica", scatter_dimension=axis, tiled=True
        )
        new, held = update(total * rate, master, memory)
        stepped.append(new)
        state.append(held)
    whole = lax.psum(partial_norm[0].astype(jnp.float32), "replica")
    size = master_norm.shape[0]
    mean = lax.dynamic_slice_in_dim(whole, lax.axis_index("replica") * size, size) * rate
    new, held = update(mean, master_norm, memory_norm)
    stepped.append(new)
    state.append(held)
    for new, axis in zip(stepped, axes + (0,)):
        compute.append(lax.all_gather(new.astype(jnp.bfloat16), "replica", axis=axis, tiled=True))
    return (*compute, *stepped, *state)


def body(*args):
    partials = [p[0] for p in args[:4]]
    partial_norm = args[4]
    masters, master_norm = args[5:9], args[9]
    memories, memory_norm = args[10:14], args[14]
    n = lax.axis_size("replica")
    shapes = {m.shape for m in masters}
    rows, cols = masters[0].shape
    fits = (
        n == MATRICES
        and len(shapes) == 1
        and rows % (32 * HALVES) == 0
        and cols % 128 == 0
        and master_norm.shape[0] == cols
    )
    form = line if fits else plain
    return form(n, partials, masters, memories, partial_norm, master_norm, memory_norm)


def solution(mesh):
    tall = P(("site", "replica"), None, "model")
    share, flat = P(("site", "replica"), "model"), P(("site", "replica"))
    wide = P(("site", "model"), "replica")
    shares = (share, share, share, wide, flat)
    return jax.shard_map(
        body,
        mesh=mesh,
        in_specs=(
            tall,
            tall,
            tall,
            P(("site", "replica"), "model", None),
            P(("site", "replica"), None),
            *shares,
            *shares,
        ),
        out_specs=(
            P("site", "model"),
            P("site", "model"),
            P("site", "model"),
            P(("site", "model"), None),
            P("site"),
            *shares,
            *shares,
        ),
        check_vma=False,
    )
```

```python
import functools

import jax
import jax.numpy as jnp
from jax import lax
from jax.experimental import pallas as pl
from jax.experimental.pallas import tpu as pltpu
from jax.sharding import PartitionSpec as P

learn_rate = 0.05
hold_rate = 0.7
HALVES = 4
DEPTH = 2
EARLY = 3
ENDS = (("raw2", 0), ("raw1", 2), ("raw3", 0), ("close", 76))
MIDDLES = (("close", 3), ("pass0", 18), ("pass2", 5), ("sum3", 1), ("sum0", 3), ("sum2", 0), ("pass3", 24))
MESH = pl.DeviceIdType.MESH
LINK = jnp.bfloat16
MATRICES = 4
LIMIT = 4.0
TOP = 125.0


def update(mean, master, memory):
    state = hold_rate * memory + (1.0 - hold_rate) * mean * mean
    return master - learn_rate * mean * lax.rsqrt(state + 1e-06), state


def encode(value, terms):
    gain = 2 * TOP / (terms * LIMIT)
    size = jnp.exp2(jnp.abs(value) * gain - TOP)
    return jnp.where(value < 0, -size, size).astype(LINK)


def decode(code, terms):
    code = code.astype(jnp.float32)
    size = (jnp.log2(jnp.abs(code)) + TOP) * (terms * LIMIT / (2 * TOP))
    return jnp.where(code < 0, -size, size)


def kernel(n, halves, *refs):
    T = MATRICES
    (partial, master, memory) = refs[0:T], refs[T : 2 * T], refs[2 * T : 3 * T]
    norms_in = refs[3 * T : 3 * T + 3]
    at = 3 * T + 3
    grown, step_v, state_v, compute_norm, stepped_norm, state_norm = refs[at : at + 6]
    (
        tall, master_v, memory_v, send_v, recv_v, norm_p, norm_m, norm_k,
        load_sem, held_sem, norm_load, rs_recv, ag_recv, end_recv, sent, raw_sent, norm_send, norm_recv,
    ) = refs[at + 6 :]
    norms_v = (norm_p, norm_m, norm_k)
    me = lax.axis_index("replica")
    rows, cols = master[0].shape
    part = rows // halves
    count = T * halves
    rate = n ** (-0.5)
    flip = jnp.where(me >= n // 2, 1, 0)
    out, back = flip, 1 - flip
    is_end = jnp.logical_or(me == 0, me == n - 1)

    def seg(s):
        return flip * (n - 1) + (1 - 2 * flip) * s

    def peer(way):
        return {"replica": me + 1 - 2 * way}

    def spot(plane, c, s):
        top = pl.multiple_of(s * rows + lax.rem(c, halves) * part, part)
        return plane.at[lax.div(c, halves), pl.ds(top, part), :]

    def loads_of(t):
        if t < T - 1:
            pairs = [(partial[t], tall.at[t])]
        else:
            pairs = [
                (partial[t].at[:, s * cols : (s + 1) * cols], tall.at[t, s * rows : (s + 1) * rows])
                for s in range(n)
            ]
        return [pltpu.make_async_copy(*pair, load_sem.at[t, i]) for i, pair in enumerate(pairs)]

    loads = [loads_of(t) for t in range(T)]
    own_norms = [
        pltpu.make_async_copy(source, target.at[me], norm_load.at[i])
        for i, (source, target) in enumerate(zip(norms_in, norms_v))
    ]
    held = [
        pltpu.make_async_copy(source[t], target.at[t], held_sem.at[i, t])
        for i, (source, target) in enumerate(((master, master_v), (memory, memory_v)))
        for t in range(T)
    ]
    for copy in loads[0]:
        copy.start()
    barrier = pltpu.get_barrier_semaphore()

    @pl.when(me > 0)
    def _():
        pl.semaphore_signal(barrier, inc=1, device_id=peer(1), device_id_type=MESH)

    @pl.when(me < n - 1)
    def _():
        pl.semaphore_signal(barrier, inc=1, device_id=peer(0), device_id_type=MESH)

    for copy in sum(loads[1:], []) + own_norms + held:
        copy.start()
    pl.semaphore_wait(barrier, jnp.where(is_end, 1, 2))

    def sum_copy(way, c, s, source):
        return pltpu.make_async_remote_copy(
            src_ref=source,
            dst_ref=recv_v.at[way, c, s],
            send_sem=sent.at[way],
            recv_sem=rs_recv.at[way, c, s],
            device_id=peer(way),
            device_id_type=MESH,
        )

    def sum_wait(way, c, s):
        sum_copy(way, c, s, send_v.at[0, c]).wait_recv()

    def share_copy(way, c, s, last=False):
        place = spot(grown, c, s)
        return pltpu.make_async_remote_copy(
            src_ref=place,
            dst_ref=place,
            send_sem=sent.at[way],
            recv_sem=end_recv.at[0] if last else ag_recv.at[way, c, s],
            device_id=peer(way),
            device_id_type=MESH,
        )

    def norm_copies(way, s):
        return [
            pltpu.make_async_remote_copy(
                src_ref=ref.at[s],
                dst_ref=ref.at[s],
                send_sem=norm_send.at[way, s, i],
                recv_sem=norm_recv.at[s, i],
                device_id=peer(way),
                device_id_type=MESH,
            )
            for i, ref in enumerate(norms_v)
        ]

    def finish(c, total, s):
        t = lax.div(c, halves)
        band = pl.ds(pl.multiple_of(lax.rem(c, halves) * part, part), part)
        new, held_new = update(total * rate, master_v[t, band, :], memory_v[t, band, :])
        spot(grown, c, s)[...] = new.astype(jnp.bfloat16)
        step_v[t, band, :] = new
        state_v[t, band, :] = held_new

    def own(c, s):
        return spot(tall, c, s)[...].astype(jnp.float32)

    def run(table, acts, low=None, high=None):
        def step(j, carry):
            for name, lag in table:
                c = j - lag

                @pl.when(jnp.logical_and(c >= 0, c < count))
                def _():
                    acts[name](c)

            return carry

        low = min(lag for _, lag in table) if low is None else low
        high = count + max(lag for _, lag in table) if high is None else high
        lax.fori_loop(low, high, step, 0)

    def sent_wait(way, planes):
        pltpu.make_async_remote_copy(
            src_ref=tall.at[0:planes],
            dst_ref=grown.at[0:planes],
            send_sem=sent.at[way],
            recv_sem=end_recv.at[0],
            device_id=peer(way),
            device_id_type=MESH,
        ).wait_send()

    @pl.when(is_end)
    def _():
        def raw_copy(c, s):
            return pltpu.make_async_remote_copy(
                src_ref=spot(tall, c, s),
                dst_ref=recv_v.at[out, c, s],
                send_sem=raw_sent.at[lax.rem(c, DEPTH), s],
                recv_sem=rs_recv.at[out, c, s],
                device_id=peer(out),
                device_id_type=MESH,
            )

        def close(c):
            sum_wait(back, c, me)
            finish(c, own(c, me) + decode(recv_v[back, c, me], n - 1), me)
            share_copy(out, c, me).start()

        def raw(s):
            def act(c):
                @pl.when(c >= DEPTH)
                def _():
                    raw_copy(c - DEPTH, seg(s)).wait_send()

                raw_copy(c, seg(s)).start()

            return act

        acts = {"raw3": raw(3), "raw2": raw(2), "raw1": raw(1), "close": close}
        for copy in loads[0]:
            copy.wait()
        first = min(lag for _, lag in ENDS)
        run(ENDS, acts, first, first + 1)
        for copy in own_norms:
            copy.wait()
        for copy in norm_copies(out, me):
            copy.start()
        run(ENDS, acts, first + 1, first + halves)
        for copy in sum(loads[1:], []) + held:
            copy.wait()
        run(ENDS, acts, first + halves)
        for s in range(1, n):
            for c in range(count - DEPTH, count):
                raw_copy(c, seg(s)).wait_send()
        for copy in norm_copies(out, me):
            copy.wait_send()
        for s in range(1, n):
            for copy in norm_copies(out, seg(s)):
                copy.wait_recv()

    @pl.when(jnp.logical_not(is_end))
    def _():
        for copy in own_norms:
            copy.wait()
        for way in range(2):
            for copy in norm_copies(way, me):
                copy.start()
        for copy in sum(loads, []) + held:
            copy.wait()

        def sum_out(s):
            def act(c):
                sum_wait(out, c, seg(s))
                total = own(c, seg(s)) + recv_v[out, c, seg(s)].astype(jnp.float32)
                send_v[s - 2, c] = encode(total, 2)
                sum_copy(out, c, seg(s), send_v.at[s - 2, c]).start()

            return act

        def sum_back(c):
            s = seg(0)
            sum_wait(back, c, s)
            send_v[2, c] = encode(own(c, s) + decode(recv_v[back, c, s], 2), 3)
            sum_copy(back, c, s, send_v.at[2, c]).start()

        def close(c):
            sum_wait(out, c, me)
            total = own(c, me) + recv_v[out, c, me].astype(jnp.float32)
            sum_wait(back, c, me)
            finish(c, total + decode(recv_v[back, c, me], 2), me)
            share_copy(out, c, me).start()
            share_copy(back, c, me, True).start()

        def pass_on(way, s, last):
            def act(c):
                share_copy(way, c, s).wait_recv()
                share_copy(way, c, s, last).start()

            return act

        acts = {
            "sum3": sum_out(3),
            "sum2": sum_out(2),
            "sum0": sum_back,
            "close": close,
            "pass0": pass_on(out, seg(0), False),
            "pass2": pass_on(back, seg(2), True),
            "pass3": pass_on(back, seg(3), True),
        }
        first = min(lag for _, lag in MIDDLES)
        run(MIDDLES, acts, first, first + EARLY)
        for way, s in ((out, 0), (back, 2)):
            for copy in norm_copies(way, seg(s)):
                copy.wait_recv()
            for copy in norm_copies(way, seg(s)):
                copy.start()
        run(MIDDLES, acts, first + EARLY, first + 2 * EARLY)
        for copy in norm_copies(back, seg(3)):
            copy.wait_recv()
        for copy in norm_copies(back, seg(3)):
            copy.start()
        run(MIDDLES, acts, first + 2 * EARLY)
        for way, s in ((out, 0), (out, 1), (back, 1), (back, 2), (back, 3)):
            for copy in norm_copies(way, seg(s)):
                copy.wait_send()

    mean = norm_p[0].astype(jnp.float32)
    for s in range(1, n):
        mean = mean + norm_p[s].astype(jnp.float32)
    mean = mean * rate
    for s in range(n):
        new, held_new = update(mean[:, s * cols : (s + 1) * cols], norm_m[s], norm_k[s])
        compute_norm[:, s * cols : (s + 1) * cols] = new

        @pl.when(me == s)
        def _():
            stepped_norm[...] = new
            state_norm[...] = held_new

    @pl.when(jnp.logical_not(is_end))
    def _():
        sent_wait(out, T)
        sent_wait(back, T)

    @pl.when(is_end)
    def _():
        sent_wait(out, 1)
        three = grown.at[0 : n - 1]
        pltpu.make_async_remote_copy(
            src_ref=three,
            dst_ref=three,
            send_sem=sent.at[out],
            recv_sem=end_recv.at[0],
            device_id=peer(out),
            device_id_type=MESH,
        ).wait_recv()


def write(n, *refs):
    T = MATRICES
    grown, step_v, state_v, compute_norm_v, stepped_norm_v, state_norm_v = refs[:6]
    compute, stepped, state = refs[6 : 6 + T], refs[6 + T : 6 + 2 * T], refs[6 + 2 * T : 6 + 3 * T]
    compute_norm, stepped_norm, state_norm, flat, sems = refs[6 + 3 * T :]
    rows, cols = stepped[0].shape
    pairs = [(grown.at[t], compute[t]) for t in range(T - 1)]
    pairs += [
        (grown.at[T - 1, s * rows : (s + 1) * rows], compute[T - 1].at[:, s * cols : (s + 1) * cols])
        for s in range(n)
    ]
    pairs += [(step_v.at[t], stepped[t]) for t in range(T)]
    pairs += [(state_v.at[t], state[t]) for t in range(T)]
    pairs += [(stepped_norm_v, stepped_norm), (state_norm_v, state_norm), (flat, compute_norm)]
    copies = [pltpu.make_async_copy(*pair, sems.at[i]) for i, pair in enumerate(pairs)]
    for copy in copies[:-1]:
        copy.start()
    flat[...] = compute_norm_v[...].reshape(flat.shape).astype(flat.dtype)
    copies[-1].start()
    for copy in copies:
        copy.wait()


def line(n, partials, masters, memories, partial_norm, master_norm, memory_norm):
    T, halves = MATRICES, HALVES
    rows, cols = masters[0].shape
    part = rows // halves
    count = T * halves
    whole = partial_norm.shape[1]
    f32, bf16 = jnp.float32, jnp.bfloat16
    anywhere = pl.BlockSpec(memory_space=pl.ANY)
    inside = pl.BlockSpec(memory_space=pltpu.VMEM)
    dma = pltpu.SemaphoreType.DMA
    kept = pl.pallas_call(
        functools.partial(kernel, n, halves),
        out_shape=[
            pltpu.VMEM((T, n * rows, cols), bf16),
            pltpu.VMEM((T, rows, cols), f32),
            pltpu.VMEM((T, rows, cols), f32),
            pltpu.VMEM((1, whole), f32),
            pltpu.VMEM((1, cols), f32),
            pltpu.VMEM((1, cols), f32),
        ],
        in_specs=[anywhere] * (3 * T + 3),
        out_specs=[inside] * 6,
        scratch_shapes=[
            pltpu.VMEM((T, n * rows, cols), bf16),
            pltpu.VMEM((T, rows, cols), f32),
            pltpu.VMEM((T, rows, cols), f32),
            pltpu.VMEM((n - 1, count, part, cols), LINK),
            pltpu.VMEM((2, count, n, part, cols), LINK),
            pltpu.VMEM((n, 1, whole), bf16),
            pltpu.VMEM((n, 1, cols), f32),
            pltpu.VMEM((n, 1, cols), f32),
            dma((T, n)),
            dma((2, T)),
            dma((3,)),
            dma((2, count, n)),
            dma((2, count, n)),
            dma((1,)),
            dma((2,)),
            dma((DEPTH, n)),
            dma((2, n, 3)),
            dma((n, 3)),
        ],
        compiler_params=pltpu.CompilerParams(
            collective_id=0, has_side_effects=True, vmem_limit_bytes=32 * 1024 * 1024
        ),
        name="line_step",
    )(
        *(
            pltpu.with_memory_space_constraint(x, pltpu.HBM)
            for x in (
                *partials, *masters, *memories, partial_norm, master_norm[None], memory_norm[None],
            )
        )
    )
    share = jax.ShapeDtypeStruct((rows, cols), f32)
    out = pl.pallas_call(
        functools.partial(write, n),
        out_shape=[jax.ShapeDtypeStruct(p.shape, bf16) for p in partials]
        + [share] * (2 * T)
        + [jax.ShapeDtypeStruct((whole,), bf16)]
        + [jax.ShapeDtypeStruct((1, cols), f32)] * 2,
        in_specs=[inside] * 6,
        out_specs=[anywhere] * (3 * T + 3),
        scratch_shapes=[pltpu.VMEM((whole,), bf16), dma((3 * T + n + 2,))],
        compiler_params=pltpu.CompilerParams(vmem_limit_bytes=1024 * 1024),
        name="write_out",
    )(*kept)
    compute, stepped, state = out[:T], out[T : 2 * T], out[2 * T : 3 * T]
    compute_norm, stepped_norm, state_norm = out[3 * T :]
    return (*compute, compute_norm, *stepped, stepped_norm[0], *state, state_norm[0])


def plain(n, partials, masters, memories, partial_norm, master_norm, memory_norm):
    rate = n ** (-0.5)
    axes = (0, 0, 0, 1)
    compute, stepped, state = [], [], []
    for p, master, memory, axis in zip(partials, masters, memories, axes):
        total = lax.psum_scatter(
            p.astype(jnp.float32), "replica", scatter_dimension=axis, tiled=True
        )
        new, held = update(total * rate, master, memory)
        stepped.append(new)
        state.append(held)
    whole = lax.psum(partial_norm[0].astype(jnp.float32), "replica")
    size = master_norm.shape[0]
    mean = lax.dynamic_slice_in_dim(whole, lax.axis_index("replica") * size, size) * rate
    new, held = update(mean, master_norm, memory_norm)
    stepped.append(new)
    state.append(held)
    for new, axis in zip(stepped, axes + (0,)):
        compute.append(lax.all_gather(new.astype(jnp.bfloat16), "replica", axis=axis, tiled=True))
    return (*compute, *stepped, *state)


def body(*args):
    partials = [p[0] for p in args[:4]]
    partial_norm = args[4]
    masters, master_norm = args[5:9], args[9]
    memories, memory_norm = args[10:14], args[14]
    n = lax.axis_size("replica")
    shapes = {m.shape for m in masters}
    rows, cols = masters[0].shape
    fits = (
        n == MATRICES
        and len(shapes) == 1
        and rows % (32 * HALVES) == 0
        and cols % 128 == 0
        and master_norm.shape[0] == cols
    )
    form = line if fits else plain
    return form(n, partials, masters, memories, partial_norm, master_norm, memory_norm)


def solution(mesh):
    tall = P(("site", "replica"), None, "model")
    share, flat = P(("site", "replica"), "model"), P(("site", "replica"))
    wide = P(("site", "model"), "replica")
    shares = (share, share, share, wide, flat)
    return jax.shard_map(
        body,
        mesh=mesh,
        in_specs=(
            tall,
            tall,
            tall,
            P(("site", "replica"), "model", None),
            P(("site", "replica"), None),
            *shares,
            *shares,
        ),
        out_specs=(
            P("site", "model"),
            P("site", "model"),
            P("site", "model"),
            P(("site", "model"), None),
            P("site"),
            *shares,
            *shares,
        ),
        check_vma=False,
    )
```
